32 devices in a mesh: tm: 4 (over y, x), users: 8 (over z, core).
Axes of the slice: x: 2, y: 2, z: 4, core: 2. Of those that a mesh axis runs over, the one named last changes fastest.
Arguments:
- features: float32 [131072, 128], P(('tm', 'users')), may hold values from -6 to 6
- home: int32 [131072, 1], P(('tm', 'users')), may hold values from 0 to 7; in each aligned block of 4096 rows (0 to 4095, 4096 to 8191, ...) at most 1024 rows name the same one
- account: int32 [131072], P(('tm', 'users')), may hold values from 0 to 127
- flags: int32 [131072], P(('tm', 'users')), may hold values 0 or 1
Outputs:
- session_mean: float32 [131072, 128], P(('tm', 'users'))
The draws below stay inside these ranges and needn't reach their ends.
Inputs may be any that keep to these rules, and one draw needn't show every extreme that they name: `home`: the 4096 events of one device name one owner at most 1024 times, a bound that some block reaches.
All inputs are finite; a program needn't handle non-finite values. No bound on the sum of `flags` on one device may be relied on, other than what follows from the above.
Results may differ from the reference program's by a relative error of at most 0.00007.
Values sent between devices are 32-bit elements; how exact they have to be, the bound alone decides.
A program may use at most 64 MiB of HBM per device.

```python
import math
import jax
import jax.numpy as jnp
import numpy as np
from jax import lax

F = 128
EV_DEV = 4096
ACCOUNTS = 128
CAP = 1024
EVENTS = 131072
N_USERS = 8


def set_ends(array, key, least, largest):
    spot = [jax.random.randint(jax.random.fold_in(key, axis), (), 0, length) for axis, length in enumerate(array.shape)]
    longest = array.shape.index(max(array.shape))
    beside = spot[:longest] + [(spot[longest] + 1) % array.shape[longest]] + spot[longest + 1:]
    return array.at[tuple(spot)].set(least).at[tuple(beside)].set(largest)


def levels(key, dims, shards, low, high):
    def one(position, shards_of):
        heights = jax.random.uniform(jax.random.fold_in(jax.random.fold_in(key, 6), position), (shards_of,), jnp.float32, low / len(shards), high / len(shards))
        return jnp.repeat(jnp.exp(heights), dims[position] // shards_of).reshape((-1,) + (1,) * (len(dims) - position - 1))

    gain = one(*shards[0])
    for cut in shards[1:]:
        gain = gain * one(*cut)
    return gain


def routed_block(key, own, number, rows, number_of, top, most, lean):
    sequence = jax.random.permutation(key, number_of)
    heavy_load, usual = load_shares(number_of, rows * top, most, lean, True), load_shares(number_of, rows * top, most, lean, False)
    places = jnp.arange(number_of)

    def named(lengths, turn):
        used = int((lengths > 0).sum())
        fixed = max(1, used // 4)
        shifted = fixed + (places - fixed + turn * (used - fixed)) % max(1, number_of - fixed)
        return jnp.zeros((number_of,), jnp.int32).at[sequence[jnp.where(places < fixed, places, shifted)]].set(jnp.asarray(lengths, jnp.int32))

    lengths = jnp.where(number % 4 == 0, named(heavy_load, number // 4), named(usual, number - number // 4 - 1))
    mixed = jax.random.permutation(jax.random.fold_in(own, 3), number_of)
    source_of, receiver = mixed[0:number_of // 2 * 2:2], mixed[1:number_of // 2 * 2:2]
    margin = jnp.minimum(lengths[source_of] - 1, most - lengths[receiver]) // 2
    margin = jnp.where((source_of == sequence[0]) | (receiver == sequence[0]) | (lengths[receiver] == 0), 0, jnp.maximum(margin, 0))
    shifted = jax.random.randint(jax.random.fold_in(own, 4), (number_of // 2,), 0, 1 << 20) % (margin + 1)
    lengths = lengths.at[source_of].add(-shifted).at[receiver].add(shifted)
    labels = jnp.searchsorted(jnp.cumsum(lengths), jnp.arange(rows * top), side="right").astype(jnp.int32)
    table = labels.reshape(top, rows).T
    table = table[jax.random.permutation(jax.random.fold_in(own, 1), rows)]
    turn = jax.random.randint(jax.random.fold_in(own, 2), (rows, 1), 0, top)
    return jnp.take_along_axis(table, (jnp.arange(top)[None, :] + turn) % top, axis=1)


def load_shares(count, total, limit, slope, full):
    weights = [(1 << 20) // math.isqrt(grade ** slope) + 1 for grade in range(1, count + 1)]
    largest = limit if full else min(limit, max(-(-total // count), total * weights[0] // sum(weights)))
    least = 1 if total - largest >= count - 1 else 0
    given, spare = [largest] + [least] * (count - 1), total - largest - least * (count - 1)
    while spare > 0:
        candidates = [i for i in range(1, count) if given[i] < largest] or [i for i in range(1, count) if given[i] < limit]
        mass, remaining = sum([weights[i] for i in candidates]), spare
        for i in candidates:
            extra = min(limit - given[i], max(1, remaining * weights[i] // mass), spare)
            given[i] = given[i] + extra
            spare = spare - extra
    return np.array(given)


def gaussian(stream_key, extent, deviation, bound, shards=(), dtype=jnp.bfloat16):
    gain = levels(stream_key, extent, shards, -0.22, 0.18) if shards else 1.0
    drawn = jax.random.normal(stream_key, extent, jnp.float32) * deviation * gain
    return jnp.minimum(jnp.maximum(drawn, -bound), bound).astype(dtype)


def setup_inputs(seed: int = 0) -> dict:
    key_list = jax.random.split(jax.random.key(seed), 5)
    features = gaussian(key_list[0], (EVENTS, F), 1.0, 6.0, ((0, 32),), jnp.float32)
    home_keys = jax.random.split(jax.random.fold_in(key_list[1], 1), EVENTS // EV_DEV)
    home_turns = jax.random.permutation(jax.random.fold_in(key_list[1], 3), EVENTS // EV_DEV)
    home = jax.vmap(lambda own, number: routed_block(jax.random.fold_in(key_list[1], 2), own, number, EV_DEV, N_USERS, 1, CAP, 2))(home_keys, home_turns).reshape((EVENTS, 1))
    account = set_ends(jax.random.randint(key_list[2], (EVENTS,), 0, ACCOUNTS), jax.random.fold_in(key_list[2], 1), 0, ACCOUNTS - 1).astype(jnp.int32)
    flags = set_ends((jax.random.randint(key_list[3], (EVENTS,), 0, 64) < 1).astype(jnp.int32), jax.random.fold_in(key_list[3], 1), 0, 1)
    return dict(features=features, home=home, account=account, flags=flags)


def combine_runs(earlier, later):
    carry_on = 1.0 - later[2]
    return (later[0] + carry_on[..., None] * earlier[0], later[1] + carry_on * earlier[1], jnp.maximum(earlier[2], later[2]))


def reference(features, home, account, flags):
    user = home[:, 0].astype(jnp.int32) * ACCOUNTS + account.astype(jnp.int32)
    order = jnp.argsort(user, stable=True)
    user_sorted = user[order]
    flag_sorted = flags[order].astype(jnp.int32)
    values = features[order]
    changed = jnp.concatenate([jnp.ones((1,), jnp.int32), (user_sorted[1:] != user_sorted[:-1]).astype(jnp.int32)])
    starts = jnp.maximum(changed, flag_sorted).astype(jnp.float32)
    singles = jnp.ones(starts.shape, jnp.float32)
    sums, counts, marks = lax.associative_scan(combine_runs, (values, singles, starts))
    means = sums / counts[:, None]
    return jnp.zeros_like(features).at[order].set(means)
```

```python
import functools
import math

import jax
import jax.numpy as jnp
from jax import lax
from jax.experimental import pallas as pl
from jax.experimental.pallas import tpu as pltpu
from jax.sharding import PartitionSpec as P

ACCOUNTS = 128
LANES = 128
TILE = ACCOUNTS + 8
VMEM_LIMIT = 60 * 1024 * 1024


def column_of(row):
    return jnp.transpose(jnp.broadcast_to(row, (LANES, LANES)))


def row_of(column):
    return jnp.transpose(column)[0:1, :]


def lane_ids(first):
    return lax.broadcasted_iota(jnp.int32, (1, LANES), 1) + first


def lane_slice(start):
    return pl.ds(pl.multiple_of(start, LANES), LANES)


def split_store(ref, rows, values):
    high = values.astype(jnp.bfloat16)
    ref[rows, 0:LANES] = high
    ref[rows, LANES : 2 * LANES] = (values - high.astype(jnp.float32)).astype(jnp.bfloat16)


def closing_states(user_ref, flag_ref, feature_ref, state_ref, halves_ref, mask_ref, fpos_ref):
    events = feature_ref.shape[0]
    chunks = events // LANES
    group = mask_ref.shape[0]
    users = state_ref.shape[1] * 2 * ACCOUNTS
    step = 4

    for chunk in range(chunks):
        at = slice(chunk * LANES, (chunk + 1) * LANES)
        fpos_ref[0:1, at] = jnp.where(flag_ref[0:1, at] > 0, lane_ids(chunk * LANES + 1), 0)

    @pl.loop(0, chunks)
    def _(chunk):
        at = lane_slice(chunk * LANES)
        split_store(halves_ref, at, feature_ref[at, :])

    @pl.loop(0, users // group)
    def _(block):
        @pl.loop(0, group // ACCOUNTS)
        def _(part):
            owner = block * (group // ACCOUNTS) + part
            ids = lax.broadcasted_iota(jnp.int32, (ACCOUNTS, LANES), 0) + owner * ACCOUNTS

            def latest(trip, found):
                for inner in range(step):
                    at = lane_slice((trip * step + inner) * LANES)
                    found = jnp.maximum(
                        found, jnp.where(user_ref[0:1, at] == ids, fpos_ref[0:1, at], 0)
                    )
                return found

            found = lax.fori_loop(
                0, chunks // step, latest, jnp.zeros((ACCOUNTS, LANES), jnp.int32)
            )
            last = jnp.broadcast_to(jnp.max(found, axis=1, keepdims=True), (ACCOUNTS, LANES))
            rows = lane_slice(part * ACCOUNTS)

            def build(trip, count):
                for inner in range(step):
                    first = (trip * step + inner) * LANES
                    at = lane_slice(first)
                    inside = (user_ref[0:1, at] == ids) & (lane_ids(first + 1) >= last)
                    weight = jnp.where(inside, 1.0, 0.0)
                    mask_ref[rows, at] = weight.astype(jnp.bfloat16)
                    count = count + weight
                return count

            count = lax.fori_loop(
                0, chunks // step, build, jnp.zeros((ACCOUNTS, LANES), jnp.float32)
            )
            count = jnp.broadcast_to(jnp.sum(count, axis=1, keepdims=True), (ACCOUNTS, LANES))
            marks = jnp.where(last > 0, 1.0, 0.0)
            stats = jnp.concatenate(
                [row_of(count), row_of(marks), jnp.zeros((6, LANES), jnp.float32)], axis=0
            )
            state_ref[lax.rem(owner, 2), owner // 2, ACCOUNTS:TILE, :] = stats

        total = jnp.dot(mask_ref[...], halves_ref[...], preferred_element_type=jnp.float32)
        total = total[:, 0:LANES] + total[:, LANES : 2 * LANES]
        for part in range(group // ACCOUNTS):
            owner = block * (group // ACCOUNTS) + part
            state_ref[lax.rem(owner, 2), owner // 2, 0:ACCOUNTS, :] = total[
                part * ACCOUNTS : (part + 1) * ACCOUNTS
            ]


def inside_sessions(
    user_ref, fpos_ref, halves_ref, sum_ref, count_ref, open_ref, key_ref, mask_ref, keycol_ref, cnt_ref, acc_ref
):
    events = halves_ref.shape[0]
    rows = mask_ref.shape[0]
    parts = rows // LANES
    diagonal = lax.broadcasted_iota(jnp.int32, (LANES, LANES), 1) <= lax.broadcasted_iota(
        jnp.int32, (LANES, LANES), 0
    )

    @pl.loop(0, events // rows)
    def _(block):
        base = block * rows
        for part in range(parts):
            mine = lane_slice(base + part * LANES)
            ids = column_of(user_ref[0:1, mine])

            def latest(trip, found):
                for inner in range(parts):
                    at = lane_slice(trip * rows + inner * LANES)
                    found = jnp.maximum(
                        found, jnp.where(user_ref[0:1, at] == ids, fpos_ref[0:1, at], 0)
                    )
                return found

            found = lax.fori_loop(0, block, latest, jnp.zeros((LANES, LANES), jnp.int32))
            for inner in range(part + 1):
                at = lane_slice(base + inner * LANES)
                same = user_ref[0:1, at] == ids
                if inner == part:
                    same = same & diagonal
                found = jnp.maximum(found, jnp.where(same, fpos_ref[0:1, at], 0))
            start = jnp.broadcast_to(jnp.max(found, axis=1, keepdims=True), (LANES, LANES))
            key = jnp.where(start > 0, start, -1 - ids)
            keycol_ref[part * LANES : (part + 1) * LANES, :] = key
            key_ref[0:1, mine] = row_of(key)
            open_ref[0:1, mine] = row_of(jnp.where(start > 0, -1, ids))

        for part in range(parts):
            here = slice(part * LANES, (part + 1) * LANES)
            key = keycol_ref[here, :]
            count = jnp.zeros((LANES, LANES), jnp.float32)
            for inner in range(parts):
                to = slice(inner * LANES, (inner + 1) * LANES)
                if inner > part:
                    mask_ref[here, to] = jnp.zeros((LANES, LANES), jnp.bfloat16)
                    continue
                same = key_ref[0:1, lane_slice(base + inner * LANES)] == key
                if inner == part:
                    same = same & diagonal
                weight = jnp.where(same, 1.0, 0.0)
                mask_ref[here, to] = weight.astype(jnp.bfloat16)
                count = count + weight
            cnt_ref[here, :] = count
        acc_ref[...] = jnp.dot(
            mask_ref[...],
            halves_ref[pl.ds(pl.multiple_of(base, rows), rows), :],
            preferred_element_type=jnp.float32,
        )

        @pl.loop(0, block)
        def _(trip):
            for part in range(parts):
                here = slice(part * LANES, (part + 1) * LANES)
                key = keycol_ref[here, :]
                count = cnt_ref[here, :]
                for inner in range(parts):
                    to = slice(inner * LANES, (inner + 1) * LANES)
                    weight = jnp.where(
                        key_ref[0:1, lane_slice(trip * rows + inner * LANES)] == key, 1.0, 0.0
                    )
                    mask_ref[here, to] = weight.astype(jnp.bfloat16)
                    count = count + weight
                cnt_ref[here, :] = count
            acc_ref[...] += jnp.dot(
                mask_ref[...],
                halves_ref[pl.ds(pl.multiple_of(trip * rows, rows), rows), :],
                preferred_element_type=jnp.float32,
            )

        sum_ref[pl.ds(pl.multiple_of(base, rows), rows), :] = (
            acc_ref[:, 0:LANES] + acc_ref[:, LANES : 2 * LANES]
        )
        for part in range(parts):
            here = slice(part * LANES, (part + 1) * LANES)
            count = jnp.sum(cnt_ref[here, :], axis=1, keepdims=True)
            count_ref[0:1, lane_slice(base + part * LANES)] = row_of(
                jnp.broadcast_to(count, (LANES, LANES))
            )


def sums_of(tile):
    return tile[0:ACCOUNTS, :]


def stats_of(tile):
    return tile[ACCOUNTS:TILE, :]


def follow(earlier, later):
    stats_e, stats_l = stats_of(earlier), stats_of(later)
    mark = stats_l[1:2, :]
    carry_on = 1.0 - mark
    sums = sums_of(later) + column_of(carry_on) * sums_of(earlier)
    count = stats_l[0:1, :] + carry_on * stats_e[0:1, :]
    seen = jnp.maximum(mark, stats_e[1:2, :])
    return jnp.concatenate([sums, count, seen, stats_l[2:8, :]], axis=0)


def exchange(
    groups, owners, state_ref, table_ref, count_ref,
    pair_in, chip, chip_in, time_out, time_in, back_out, back_in, pair_out, pair_back, sends, recvs,
):
    chips = owners // 2
    time, me = lax.axis_index("tm"), lax.axis_index("users")
    core, z = lax.rem(me, 2), me // 2
    sibling = me + 1 - 2 * core
    other = 1 - core
    zeros = jnp.zeros((TILE, LANES), jnp.float32)

    def copy(source, target, stage, mine, theirs, device):
        return pltpu.make_async_remote_copy(
            src_ref=source,
            dst_ref=target,
            send_sem=sends.at[stage, mine],
            recv_sem=recvs.at[stage, theirs],
            device_id=device,
            device_id_type=pl.DeviceIdType.MESH,
        )

    def peer(shift):
        return lax.rem(z + shift, chips)

    def each(first, last, fn):
        if last - first <= 8:
            for index in range(first, last):
                fn(index)
        else:
            pl.loop(first, last)(fn)

    def device(group, user):
        return (group, user)

    barrier = pltpu.get_barrier_semaphore()
    pl.semaphore_signal(barrier, inc=1, device_id=device(time, sibling), device_id_type=pl.DeviceIdType.MESH)
    each(1, chips, lambda k: pl.semaphore_signal(
        barrier, inc=1, device_id=device(time, 2 * peer(k) + core), device_id_type=pl.DeviceIdType.MESH))
    each(1, groups, lambda k: pl.semaphore_signal(
        barrier, inc=1, device_id=device(lax.rem(time + k, groups), me), device_id_type=pl.DeviceIdType.MESH))
    pl.semaphore_wait(barrier, 1 + (chips - 1) + (groups - 1))

    def swap(k):
        to = peer(k)
        copy(state_ref.at[other, to], pair_in.at[to], 0, to, to, device(time, sibling)).start()

    each(1, chips, swap)
    swap(0)

    def gather(k):
        to = peer(k)
        got = copy(state_ref.at[other, to], pair_in.at[to], 0, to, to, device(time, sibling))
        got.wait_recv()
        mine, theirs = state_ref[core, to], pair_in[to]
        first = core == 0
        chip[to] = follow(jnp.where(first, mine, theirs), jnp.where(first, theirs, mine))

    def to_owner(k):
        to = peer(k)
        return copy(chip.at[to], chip_in.at[z], 1, to, z, device(time, 2 * to + core))

    def gather_send(k):
        gather(k)
        to_owner(k).start()

    each(1, chips, gather_send)
    gather(0)
    chip_in[z] = chip[z]

    def from_owner(k):
        source = peer(k)
        copy(chip.at[source], chip_in.at[source], 1, source, source, device(time, 2 * source + core)).wait_recv()

    each(1, chips, from_owner)

    total = lax.fori_loop(0, chips, lambda at, so_far: follow(so_far, chip_in[at]), zeros)
    time_out[...] = total

    def to_time(k):
        to = lax.rem(time + k, groups)
        return copy(time_out, time_in.at[time], 2, to, time, device(to, me))

    each(1, groups, lambda k: to_time(k).start())
    time_in[time] = zeros

    def from_time(k):
        source = lax.rem(time + k, groups)
        copy(time_out, time_in.at[source], 2, source, source, device(source, me)).wait_recv()

    each(1, groups, from_time)

    def advance(at, so_far):
        return jnp.where(at < time, follow(so_far, time_in[at]), so_far)

    incoming = lax.fori_loop(0, groups, advance, zeros)

    def prefixes(at, so_far):
        back_out[at] = so_far
        return follow(so_far, chip_in[at])

    lax.fori_loop(0, chips, prefixes, incoming)

    def to_chip(k):
        to = peer(k)
        return copy(back_out.at[to], back_in.at[z], 3, to, z, device(time, 2 * to + core))

    each(1, chips, lambda k: to_chip(k).start())
    back_in[z] = back_out[z]

    def finish(half, at, tile):
        owner = 2 * at + half
        split_store(table_ref, lane_slice(owner * ACCOUNTS), sums_of(tile))
        count_ref[0:1, lane_slice(owner * ACCOUNTS)] = stats_of(tile)[0:1, :]

    def to_sibling(at):
        return copy(pair_out.at[at], pair_back.at[at], 4, at, at, device(time, sibling))

    def hand_over(k):
        at = peer(k)
        tile = back_in[at]
        first = core == 0
        after = follow(tile, jnp.where(first, state_ref[core, at], pair_in[at]))
        pair_out[at] = jnp.where(first, after, tile)
        to_sibling(at).start()
        finish(core, at, jnp.where(first, tile, after))

    def wait_hand_over(k):
        source = peer(k)
        copy(back_out.at[source], back_in.at[source], 3, source, source, device(time, 2 * source + core)).wait_recv()
        hand_over(k)

    hand_over(0)
    each(1, chips, wait_hand_over)

    def last(k):
        at = peer(k)
        to_sibling(at).wait_recv()
        finish(other, at, pair_back[at])

    each(0, chips, last)

    def drain(k):
        to = peer(k)
        to_owner(k).wait_send()
        to_chip(k).wait_send()

    def drain_pair(k):
        to = peer(k)
        copy(state_ref.at[other, to], pair_in.at[to], 0, to, to, device(time, sibling)).wait_send()
        to_sibling(to).wait_send()

    each(1, chips, drain)
    each(0, chips, drain_pair)
    each(1, groups, lambda k: to_time(k).wait_send())


def means(open_ref, own_ref, sum_ref, table_ref, count_ref, out_ref, mask_ref):
    rows, users = mask_ref.shape
    counts = []
    for part in range(rows // LANES):
        here = slice(part * LANES, (part + 1) * LANES)
        ids = column_of(open_ref[0:1, here])

        def build(chunk, count):
            at = lane_slice(chunk * LANES)
            same = lane_ids(chunk * LANES) == ids
            mask_ref[here, at] = jnp.where(same, 1.0, 0.0).astype(jnp.bfloat16)
            return count + jnp.where(same, count_ref[0:1, at], 0.0)

        count = lax.fori_loop(
            0, users // LANES, build, jnp.zeros((LANES, LANES), jnp.float32), unroll=users <= 1024
        )
        counts.append(jnp.sum(count, axis=1, keepdims=True) + column_of(own_ref[0:1, here]))
    before = jnp.dot(mask_ref[...], table_ref[...], preferred_element_type=jnp.float32)
    before = before[:, 0:LANES] + before[:, LANES : 2 * LANES]
    out_ref[...] = (sum_ref[...] + before) / jnp.concatenate(counts, axis=0)


def local_kernel(user_ref, flag_ref, feature_ref, state_ref, sum_ref, count_ref, open_ref,
                 halves, fpos, mask, key, mask2, keycol, cnt, acc):
    closing_states(user_ref, flag_ref, feature_ref, state_ref, halves, mask, fpos)
    inside_sessions(user_ref, fpos, halves, sum_ref, count_ref, open_ref, key, mask2, keycol, cnt, acc)


def body(groups, owners, features, home, account, flags):
    events = features.shape[0]
    users = owners * ACCOUNTS
    chips = owners // 2
    rows = math.gcd(events, 512)
    group = math.gcd(users, 512)
    whole = pl.BlockSpec(memory_space=pltpu.VMEM)
    user = home.reshape(1, events) * ACCOUNTS + account.reshape(1, events)

    state, own_sum, own_count, open_user = pl.pallas_call(
        local_kernel,
        out_shape=(
            jax.ShapeDtypeStruct((2, chips, TILE, LANES), jnp.float32),
            jax.ShapeDtypeStruct((events, LANES), jnp.float32),
            jax.ShapeDtypeStruct((1, events), jnp.float32),
            jax.ShapeDtypeStruct((1, events), jnp.int32),
        ),
        in_specs=[whole] * 3,
        out_specs=(whole,) * 4,
        scratch_shapes=[
            pltpu.VMEM((events, 2 * LANES), jnp.bfloat16),
            pltpu.VMEM((1, events), jnp.int32),
            pltpu.VMEM((group, events), jnp.bfloat16),
            pltpu.VMEM((1, events), jnp.int32),
            pltpu.VMEM((rows, rows), jnp.bfloat16),
            pltpu.VMEM((rows, LANES), jnp.int32),
            pltpu.VMEM((rows, LANES), jnp.float32),
            pltpu.VMEM((rows, 2 * LANES), jnp.float32),
        ],
        compiler_params=pltpu.CompilerParams(vmem_limit_bytes=VMEM_LIMIT),
        name="local",
    )(user, flags.reshape(1, events), features)

    tiles = lambda count: pltpu.VMEM((count, TILE, LANES), jnp.float32)
    lots = max(chips, groups)
    table, prefix_count = pl.pallas_call(
        functools.partial(exchange, groups, owners),
        out_shape=(
            jax.ShapeDtypeStruct((users, 2 * LANES), jnp.bfloat16),
            jax.ShapeDtypeStruct((1, users), jnp.float32),
        ),
        in_specs=[whole],
        out_specs=(whole,) * 2,
        scratch_shapes=[
            tiles(chips), tiles(chips), tiles(chips),
            pltpu.VMEM((TILE, LANES), jnp.float32), tiles(groups),
            tiles(chips), tiles(chips), tiles(chips), tiles(chips),
            pltpu.SemaphoreType.DMA((5, lots)),
            pltpu.SemaphoreType.DMA((5, lots)),
        ],
        compiler_params=pltpu.CompilerParams(
            collective_id=0, has_side_effects=True, vmem_limit_bytes=VMEM_LIMIT
        ),
        name="exchange",
    )(state)

    return pl.pallas_call(
        means,
        grid=(events // rows,),
        out_shape=jax.ShapeDtypeStruct((events, LANES), jnp.float32),
        in_specs=[
            pl.BlockSpec((1, rows), lambda i: (0, i)),
            pl.BlockSpec((1, rows), lambda i: (0, i)),
            pl.BlockSpec((rows, LANES), lambda i: (i, 0)),
            pl.BlockSpec((users, 2 * LANES), lambda i: (0, 0)),
            pl.BlockSpec((1, users), lambda i: (0, 0)),
        ],
        out_specs=pl.BlockSpec((rows, LANES), lambda i: (i, 0)),
        scratch_shapes=[pltpu.VMEM((rows, users), jnp.bfloat16)],
        compiler_params=pltpu.CompilerParams(vmem_limit_bytes=VMEM_LIMIT),
        name="means",
    )(open_user, own_count, own_sum, table, prefix_count)


def solution(mesh):
    return jax.shard_map(
        functools.partial(body, mesh.shape["tm"], mesh.shape["users"]),
        mesh=mesh,
        in_specs=(
            P(("tm", "users"), None),
            P(("tm", "users"), None),
            P(("tm", "users")),
            P(("tm", "users")),
        ),
        out_specs=P(("tm", "users"), None),
        check_vma=False,
    )
```

```python
import functools
import math

import jax
import jax.numpy as jnp
from jax import lax
from jax.experimental import pallas as pl
from jax.experimental.pallas import tpu as pltpu
from jax.sharding import PartitionSpec as P

ACCOUNTS = 128
LANES = 128
TILE = ACCOUNTS + 8
VMEM_LIMIT = 60 * 1024 * 1024


def column_of(row):
    return jnp.transpose(jnp.broadcast_to(row, (LANES, LANES)))


def row_of(column):
    return jnp.transpose(column)[0:1, :]


def lane_ids(first):
    return lax.broadcasted_iota(jnp.int32, (1, LANES), 1) + first


def lane_slice(start):
    return pl.ds(pl.multiple_of(start, LANES), LANES)


def split_store(ref, rows, values):
    high = values.astype(jnp.bfloat16)
    ref[rows, 0:LANES] = high
    ref[rows, LANES : 2 * LANES] = (values - high.astype(jnp.float32)).astype(jnp.bfloat16)


def stacked(rows16):
    return jnp.concatenate([rows16] * (LANES // 16), axis=0)


def short(values):
    return values.astype(jnp.int16)


def one_if(condition):
    return jnp.where(condition, jnp.bfloat16(1), jnp.bfloat16(0))


def prepare(home_ref, account_ref, flag_ref, feature_ref, halves_ref, user_ref, user16_ref, flagged16_ref, pos16_ref):
    chunks = feature_ref.shape[0] // LANES
    step = math.gcd(chunks, 4)

    @pl.loop(0, chunks // step)
    def _(trip):
        for inner in range(step):
            chunk = trip * step + inner
            at = lane_slice(chunk * LANES)
            pos = lane_ids(chunk * LANES + 1)
            user = home_ref[0:1, at] * ACCOUNTS + account_ref[0:1, at]
            flagged = jnp.where(flag_ref[0:1, at] > 0, user, -1)
            user_ref[0:1, at] = user
            user16_ref[:, at] = short(jnp.broadcast_to(user, (16, LANES)))
            flagged16_ref[:, at] = short(jnp.broadcast_to(flagged, (16, LANES)))
            pos16_ref[:, at] = short(jnp.broadcast_to(pos, (16, LANES)))
            split_store(halves_ref, at, feature_ref[at, :])


def row_max(found):
    return jnp.max(jnp.transpose(found.astype(jnp.int32)), axis=0, keepdims=True)


def row_sum(values):
    return jnp.sum(jnp.transpose(values.astype(jnp.float32)), axis=0, keepdims=True)


def closing_states(halves_ref, user16_ref, flagged16_ref, pos16_ref, state_ref, mask_ref, last_ref):
    events = halves_ref.shape[0]
    chunks = events // LANES
    group = mask_ref.shape[0]
    parts = group // ACCOUNTS
    users = state_ref.shape[1] * 2 * ACCOUNTS
    step = math.gcd(chunks, 8)

    @pl.loop(0, users // group)
    def _(block):
        def ids_of(part):
            return short(
                lax.broadcasted_iota(jnp.int32, (ACCOUNTS, LANES), 0)
                + (block * parts + part) * ACCOUNTS
            )

        def latest(trip, found):
            for inner in range(step):
                at = lane_slice((trip * step + inner) * LANES)
                flagged, pos = stacked(flagged16_ref[:, at]), stacked(pos16_ref[:, at])
                found = tuple(
                    jnp.where(flagged == ids_of(part), pos, found[part]) for part in range(parts)
                )
            return found

        found = lax.fori_loop(
            0, chunks // step, latest, (jnp.zeros((ACCOUNTS, LANES), jnp.int16),) * parts
        )
        marks = []
        for part in range(parts):
            last = row_max(found[part])
            marks.append(jnp.where(last > 0, 1.0, 0.0))
            last_ref[part * LANES : (part + 1) * LANES, :] = short(column_of(last))

        def build(trip, count):
            for inner in range(step):
                at = lane_slice((trip * step + inner) * LANES)
                user, pos = stacked(user16_ref[:, at]), stacked(pos16_ref[:, at])
                grown = []
                for part in range(parts):
                    here = slice(part * LANES, (part + 1) * LANES)
                    weight = one_if((user == ids_of(part)) & (pos >= last_ref[here, :]))
                    mask_ref[here, at] = weight
                    grown.append(count[part] + weight)
                count = tuple(grown)
            return count

        count = lax.fori_loop(
            0, chunks // step, build, (jnp.zeros((ACCOUNTS, LANES), jnp.bfloat16),) * parts
        )
        total = jnp.dot(mask_ref[...], halves_ref[...], preferred_element_type=jnp.float32)
        total = total[:, 0:LANES] + total[:, LANES : 2 * LANES]
        for part in range(parts):
            owner = block * parts + part
            half, at = lax.rem(owner, 2), owner // 2
            state_ref[half, at, ACCOUNTS:TILE, :] = jnp.concatenate(
                [row_sum(count[part]), marks[part], jnp.zeros((6, LANES), jnp.float32)], axis=0
            )
            state_ref[half, at, 0:ACCOUNTS, :] = total[part * ACCOUNTS : (part + 1) * ACCOUNTS]


def inside_sessions(
    first_block, end_block, halves_ref, user_ref, flagged16_ref, pos16_ref,
    sum_ref, count_ref, open_ref, key16_ref, mask_ref, keycol_ref, cnt_ref, acc_ref
):
    rows = acc_ref.shape[0]
    parts = rows // LANES
    diagonal = short(lax.broadcasted_iota(jnp.int32, (LANES, LANES), 1)) <= short(
        lax.broadcasted_iota(jnp.int32, (LANES, LANES), 0)
    )

    @pl.loop(first_block, end_block)
    def _(block):
        base = block * rows
        here = [slice(part * LANES, (part + 1) * LANES) for part in range(parts)]
        mine = [lane_slice(base + part * LANES) for part in range(parts)]
        for part in range(parts):
            keycol_ref[here[part], :] = short(column_of(user_ref[0:1, mine[part]]))

        def latest(trip, found):
            for inner in range(parts):
                at = lane_slice(trip * rows + inner * LANES)
                flagged, pos = stacked(flagged16_ref[:, at]), stacked(pos16_ref[:, at])
                found = tuple(
                    jnp.where(flagged == keycol_ref[here[part], :], pos, found[part])
                    for part in range(parts)
                )
            return found

        found = lax.fori_loop(
            0, block, latest, (jnp.zeros((LANES, LANES), jnp.int16),) * parts
        )
        keys = []
        for part in range(parts):
            seen = found[part]
            for inner in range(part + 1):
                same = stacked(flagged16_ref[:, mine[inner]]) == keycol_ref[here[part], :]
                if inner == part:
                    same = same & diagonal
                seen = jnp.where(same, stacked(pos16_ref[:, mine[inner]]), seen)
            start = row_max(seen)
            user = user_ref[0:1, mine[part]]
            key = jnp.where(start > 0, start, -1 - user)
            keys.append(key)
            open_ref[0:1, mine[part]] = jnp.where(start > 0, -1, user)
        for part in range(parts):
            keycol_ref[here[part], :] = short(column_of(keys[part]))
            key16_ref[:, mine[part]] = short(jnp.broadcast_to(keys[part], (16, LANES)))

        for part in range(parts):
            key = keycol_ref[here[part], :]
            count = jnp.zeros((LANES, LANES), jnp.bfloat16)
            for inner in range(parts):
                if inner > part:
                    mask_ref[here[part], here[inner]] = jnp.zeros((LANES, LANES), jnp.bfloat16)
                    continue
                same = stacked(key16_ref[:, mine[inner]]) == key
                if inner == part:
                    same = same & diagonal
                weight = one_if(same)
                mask_ref[here[part], here[inner]] = weight
                count = count + weight
            cnt_ref[here[part], :] = count
        acc_ref[...] = jnp.dot(
            mask_ref[0:rows, 0:rows],
            halves_ref[pl.ds(pl.multiple_of(base, rows), rows), :],
            preferred_element_type=jnp.float32,
        )

        @pl.loop(0, block)
        def _(trip):
            for part in range(parts):
                key = keycol_ref[here[part], :]
                count = cnt_ref[here[part], :]
                for inner in range(parts):
                    at = lane_slice(trip * rows + inner * LANES)
                    weight = one_if(stacked(key16_ref[:, at]) == key)
                    mask_ref[here[part], here[inner]] = weight
                    count = count + weight
                cnt_ref[here[part], :] = count
            acc_ref[...] += jnp.dot(
                mask_ref[0:rows, 0:rows],
                halves_ref[pl.ds(pl.multiple_of(trip * rows, rows), rows), :],
                preferred_element_type=jnp.float32,
            )

        sum_ref[pl.ds(pl.multiple_of(base, rows), rows), :] = (
            acc_ref[:, 0:LANES] + acc_ref[:, LANES : 2 * LANES]
        )
        for part in range(parts):
            count_ref[0:1, mine[part]] = row_sum(cnt_ref[here[part], :])


def sums_of(tile):
    return tile[0:ACCOUNTS, :]


def stats_of(tile):
    return tile[ACCOUNTS:TILE, :]


def follow(earlier, later):
    stats_e, stats_l = stats_of(earlier), stats_of(later)
    mark = stats_l[1:2, :]
    carry_on = 1.0 - mark
    sums = sums_of(later) + column_of(carry_on) * sums_of(earlier)
    count = stats_l[0:1, :] + carry_on * stats_e[0:1, :]
    seen = jnp.maximum(mark, stats_e[1:2, :])
    return jnp.concatenate([sums, count, seen, stats_l[2:8, :]], axis=0)


def exchange(
    groups, owners, home_ref, account_ref, flag_ref, feature_ref,
    table_ref, count_ref, sum_ref, own_count_ref, open_ref,
    state_ref, halves, user_ref, user16, flagged16, pos16, key16, mask, last, keycol, cnt, acc,
    pair_in, chip, chip_in, time_out, time_in, back_out, back_in, pair_out, pair_back, sends, recvs,
):
    chips = owners // 2
    time, me = lax.axis_index("tm"), lax.axis_index("users")
    core, z = lax.rem(me, 2), me // 2
    sibling = me + 1 - 2 * core
    other = 1 - core
    zeros = jnp.zeros((TILE, LANES), jnp.float32)

    def copy(source, target, stage, mine, theirs, device):
        return pltpu.make_async_remote_copy(
            src_ref=source,
            dst_ref=target,
            send_sem=sends.at[stage, mine],
            recv_sem=recvs.at[stage, theirs],
            device_id=device,
            device_id_type=pl.DeviceIdType.MESH,
        )

    def peer(shift):
        return lax.rem(z + shift, chips)

    def each(first, last, fn):
        if last - first <= 8:
            for index in range(first, last):
                fn(index)
        else:
            pl.loop(first, last)(fn)

    def device(group, user):
        return (group, user)

    barrier = pltpu.get_barrier_semaphore()
    pl.semaphore_signal(barrier, inc=1, device_id=device(time, sibling), device_id_type=pl.DeviceIdType.MESH)
    each(1, chips, lambda k: pl.semaphore_signal(
        barrier, inc=1, device_id=device(time, 2 * peer(k) + core), device_id_type=pl.DeviceIdType.MESH))
    each(1, groups, lambda k: pl.semaphore_signal(
        barrier, inc=1, device_id=device(lax.rem(time + k, groups), me), device_id_type=pl.DeviceIdType.MESH))

    prepare(home_ref, account_ref, flag_ref, feature_ref, halves, user_ref, user16, flagged16, pos16)
    closing_states(halves, user16, flagged16, pos16, state_ref, mask, last)
    blocks = sum_ref.shape[0] // acc.shape[0]
    early = blocks * 5 // 8

    def inside(first, end):
        inside_sessions(first, end, halves, user_ref, flagged16, pos16,
                        sum_ref, own_count_ref, open_ref, key16, mask, keycol, cnt, acc)

    pl.semaphore_wait(barrier, 1 + (chips - 1) + (groups - 1))

    def swap(k):
        to = peer(k)
        copy(state_ref.at[other, to], pair_in.at[to], 0, to, to, device(time, sibling)).start()

    each(1, chips, swap)
    swap(0)

    def gather(k):
        to = peer(k)
        got = copy(state_ref.at[other, to], pair_in.at[to], 0, to, to, device(time, sibling))
        got.wait_recv()
        mine, theirs = state_ref[core, to], pair_in[to]
        first = core == 0
        chip[to] = follow(jnp.where(first, mine, theirs), jnp.where(first, theirs, mine))

    def to_owner(k):
        to = peer(k)
        return copy(chip.at[to], chip_in.at[z], 1, to, z, device(time, 2 * to + core))

    def gather_send(k):
        gather(k)
        to_owner(k).start()

    each(1, chips, gather_send)
    gather(0)
    chip_in[z] = chip[z]
    inside(0, early)

    def from_owner(k):
        source = peer(k)
        copy(chip.at[source], chip_in.at[source], 1, source, source, device(time, 2 * source + core)).wait_recv()

    each(1, chips, from_owner)

    total = lax.fori_loop(0, chips, lambda at, so_far: follow(so_far, chip_in[at]), zeros)
    time_out[...] = total

    def to_time(k):
        to = lax.rem(time + k, groups)
        return copy(time_out, time_in.at[time], 2, to, time, device(to, me))

    each(1, groups, lambda k: to_time(k).start())
    time_in[time] = zeros

    def from_time(k):
        source = lax.rem(time + k, groups)
        copy(time_out, time_in.at[source], 2, source, source, device(source, me)).wait_recv()

    each(1, groups, from_time)

    def advance(at, so_far):
        return jnp.where(at < time, follow(so_far, time_in[at]), so_far)

    incoming = lax.fori_loop(0, groups, advance, zeros)

    def prefixes(at, so_far):
        back_out[at] = so_far
        return follow(so_far, chip_in[at])

    lax.fori_loop(0, chips, prefixes, incoming)

    def to_chip(k):
        to = peer(k)
        return copy(back_out.at[to], back_in.at[z], 3, to, z, device(time, 2 * to + core))

    each(1, chips, lambda k: to_chip(k).start())
    back_in[z] = back_out[z]
    inside(early, blocks)

    def finish(half, at, tile):
        owner = 2 * at + half
        split_store(table_ref, lane_slice(owner * ACCOUNTS), sums_of(tile))
        count_ref[0:1, lane_slice(owner * ACCOUNTS)] = stats_of(tile)[0:1, :]

    def to_sibling(at):
        return copy(pair_out.at[at], pair_back.at[at], 4, at, at, device(time, sibling))

    def hand_over(k):
        at = peer(k)
        tile = back_in[at]
        first = core == 0
        after = follow(tile, jnp.where(first, state_ref[core, at], pair_in[at]))
        pair_out[at] = jnp.where(first, after, tile)
        to_sibling(at).start()
        finish(core, at, jnp.where(first, tile, after))

    def wait_hand_over(k):
        source = peer(k)
        copy(back_out.at[source], back_in.at[source], 3, source, source, device(time, 2 * source + core)).wait_recv()
        hand_over(k)

    hand_over(0)
    each(1, chips, wait_hand_over)

    def last(k):
        at = peer(k)
        to_sibling(at).wait_recv()
        finish(other, at, pair_back[at])

    each(0, chips, last)

    def drain(k):
        to = peer(k)
        to_owner(k).wait_send()
        to_chip(k).wait_send()

    def drain_pair(k):
        to = peer(k)
        copy(state_ref.at[other, to], pair_in.at[to], 0, to, to, device(time, sibling)).wait_send()
        to_sibling(to).wait_send()

    each(1, chips, drain)
    each(0, chips, drain_pair)
    each(1, groups, lambda k: to_time(k).wait_send())


def means(open_ref, own_ref, sum_ref, table_ref, count_ref, out_ref, mask_ref):
    rows, users = mask_ref.shape
    high = (count_ref[...] * (1.0 / 32768.0)).astype(jnp.int32)
    low = count_ref[...].astype(jnp.int32) - high * 32768
    counts = []
    for part in range(rows // LANES):
        here = slice(part * LANES, (part + 1) * LANES)
        ids = short(column_of(open_ref[0:1, here]))

        def build(chunk, found, rows_of):
            at = lane_slice(chunk * LANES)
            same = short(jnp.broadcast_to(lane_ids(chunk * LANES), (LANES, LANES))) == ids
            mask_ref[here, at] = one_if(same)
            return tuple(
                jnp.where(same, short(jnp.broadcast_to(row, (LANES, LANES))), so_far)
                for row, so_far in zip(rows_of(chunk), found)
            )

        found = (jnp.zeros((LANES, LANES), jnp.int16),) * 2
        if users <= 1024:
            for chunk in range(users // LANES):
                at = slice(chunk * LANES, (chunk + 1) * LANES)
                found = build(chunk, found, lambda chunk: (high[:, at], low[:, at]))
        else:
            def pieces(chunk):
                count = count_ref[0:1, lane_slice(chunk * LANES)]
                upper = (count * (1.0 / 32768.0)).astype(jnp.int32)
                return upper, count.astype(jnp.int32) - upper * 32768

            found = lax.fori_loop(
                0, users // LANES, lambda chunk, found: build(chunk, found, pieces), found
            )
        count = found[0].astype(jnp.int32) * 32768 + found[1].astype(jnp.int32)
        counts.append(row_sum(count) + own_ref[0:1, here])
    before = jnp.dot(mask_ref[...], table_ref[...], preferred_element_type=jnp.float32)
    before = before[:, 0:LANES] + before[:, LANES : 2 * LANES]
    for part in range(rows // LANES):
        here = slice(part * LANES, (part + 1) * LANES)
        out_ref[here, :] = (sum_ref[here, :] + before[here]) / column_of(counts[part])


def body(groups, owners, features, home, account, flags):
    events = features.shape[0]
    users = owners * ACCOUNTS
    chips = owners // 2
    rows = math.gcd(events, 512)
    group = math.gcd(users, 512)
    whole = pl.BlockSpec(memory_space=pltpu.VMEM)
    tiles = lambda *count: pltpu.VMEM((*count, TILE, LANES), jnp.float32)
    lots = max(chips, groups)
    table, prefix_count, own_sum, own_count, open_user = pl.pallas_call(
        functools.partial(exchange, groups, owners),
        out_shape=(
            jax.ShapeDtypeStruct((users, 2 * LANES), jnp.bfloat16),
            jax.ShapeDtypeStruct((1, users), jnp.float32),
            jax.ShapeDtypeStruct((events, LANES), jnp.float32),
            jax.ShapeDtypeStruct((1, events), jnp.float32),
            jax.ShapeDtypeStruct((1, events), jnp.int32),
        ),
        in_specs=[whole] * 4,
        out_specs=(whole,) * 5,
        scratch_shapes=[
            tiles(2, chips),
            pltpu.VMEM((events, 2 * LANES), jnp.bfloat16),
            pltpu.VMEM((1, events), jnp.int32),
            pltpu.VMEM((16, events), jnp.int16),
            pltpu.VMEM((16, events), jnp.int16),
            pltpu.VMEM((16, events), jnp.int16),
            pltpu.VMEM((16, events), jnp.int16),
            pltpu.VMEM((group, events), jnp.bfloat16),
            pltpu.VMEM((group, LANES), jnp.int16),
            pltpu.VMEM((rows, LANES), jnp.int16),
            pltpu.VMEM((rows, LANES), jnp.bfloat16),
            pltpu.VMEM((rows, 2 * LANES), jnp.float32),
            tiles(chips), tiles(chips), tiles(chips),
            tiles(), tiles(groups),
            tiles(chips), tiles(chips), tiles(chips), tiles(chips),
            pltpu.SemaphoreType.DMA((5, lots)),
            pltpu.SemaphoreType.DMA((5, lots)),
        ],
        compiler_params=pltpu.CompilerParams(
            collective_id=0, has_side_effects=True, vmem_limit_bytes=VMEM_LIMIT
        ),
        name="exchange",
    )(home.reshape(1, events), account.reshape(1, events), flags.reshape(1, events), features)

    return pl.pallas_call(
        means,
        grid=(events // rows,),
        out_shape=jax.ShapeDtypeStruct((events, LANES), jnp.float32),
        in_specs=[
            pl.BlockSpec((1, rows), lambda i: (0, i)),
            pl.BlockSpec((1, rows), lambda i: (0, i)),
            pl.BlockSpec((rows, LANES), lambda i: (i, 0)),
            pl.BlockSpec((users, 2 * LANES), lambda i: (0, 0)),
            pl.BlockSpec((1, users), lambda i: (0, 0)),
        ],
        out_specs=pl.BlockSpec((rows, LANES), lambda i: (i, 0)),
        scratch_shapes=[pltpu.VMEM((rows, users), jnp.bfloat16)],
        compiler_params=pltpu.CompilerParams(vmem_limit_bytes=VMEM_LIMIT),
        name="means",
    )(open_user, own_count, own_sum, table, prefix_count)


def solution(mesh):
    return jax.shard_map(
        functools.partial(body, mesh.shape["tm"], mesh.shape["users"]),
        mesh=mesh,
        in_specs=(
            P(("tm", "users"), None),
            P(("tm", "users"), None),
            P(("tm", "users")),
            P(("tm", "users")),
        ),
        out_specs=P(("tm", "users"), None),
        check_vma=False,
    )
```

```python
import functools
import math

import jax
import jax.numpy as jnp
from jax import lax
from jax.experimental import pallas as pl
from jax.experimental.pallas import tpu as pltpu
from jax.sharding import PartitionSpec as P

ACCOUNTS = 128
LANES = 128
TILE = ACCOUNTS + 8
VMEM_LIMIT = 60 * 1024 * 1024


def column_of(row):
    return jnp.transpose(jnp.broadcast_to(row, (LANES, LANES)))


def row_of(column):
    return jnp.transpose(column)[0:1, :]


def lane_ids(first):
    return lax.broadcasted_iota(jnp.int32, (1, LANES), 1) + first


def lane_slice(start):
    return pl.ds(pl.multiple_of(start, LANES), LANES)


def split_store(ref, rows, values):
    high = values.astype(jnp.bfloat16)
    ref[rows, 0:LANES] = high
    ref[rows, LANES : 2 * LANES] = (values - high.astype(jnp.float32)).astype(jnp.bfloat16)


def stacked(rows16):
    return jnp.concatenate([rows16] * (LANES // 16), axis=0)


def short(values):
    return values.astype(jnp.int16)


def one_if(condition):
    return jnp.where(condition, jnp.bfloat16(1), jnp.bfloat16(0))


def prepare(home_ref, account_ref, flag_ref, feature_ref, halves_ref, user_ref, user16_ref, flagged16_ref, pos16_ref):
    chunks = feature_ref.shape[0] // LANES
    step = math.gcd(chunks, 4)

    @pl.loop(0, chunks // step)
    def _(trip):
        for inner in range(step):
            chunk = trip * step + inner
            at = lane_slice(chunk * LANES)
            pos = lane_ids(chunk * LANES + 1)
            user = home_ref[0:1, at] * ACCOUNTS + account_ref[0:1, at]
            flagged = jnp.where(flag_ref[0:1, at] > 0, user, -1)
            user_ref[0:1, at] = user
            user16_ref[:, at] = short(jnp.broadcast_to(user, (16, LANES)))
            flagged16_ref[:, at] = short(jnp.broadcast_to(flagged, (16, LANES)))
            pos16_ref[:, at] = short(jnp.broadcast_to(pos, (16, LANES)))
            split_store(halves_ref, at, feature_ref[at, :])


def row_max(found):
    return jnp.max(jnp.transpose(found.astype(jnp.int32)), axis=0, keepdims=True)


def row_sum(values):
    return jnp.sum(jnp.transpose(values.astype(jnp.float32)), axis=0, keepdims=True)


def closing_states(halves_ref, user16_ref, flagged16_ref, pos16_ref, state_ref, mask_ref, last_ref):
    events = halves_ref.shape[0]
    chunks = events // LANES
    group = mask_ref.shape[0]
    parts = group // ACCOUNTS
    users = state_ref.shape[1] * 2 * ACCOUNTS
    step = math.gcd(chunks, 8)

    @pl.loop(0, users // group)
    def _(block):
        def ids_of(part):
            return short(
                lax.broadcasted_iota(jnp.int32, (ACCOUNTS, LANES), 0)
                + (block * parts + part) * ACCOUNTS
            )

        def latest(trip, found):
            for inner in range(step):
                at = lane_slice((trip * step + inner) * LANES)
                flagged, pos = stacked(flagged16_ref[:, at]), stacked(pos16_ref[:, at])
                found = tuple(
                    jnp.where(flagged == ids_of(part), pos, found[part]) for part in range(parts)
                )
            return found

        found = lax.fori_loop(
            0, chunks // step, latest, (jnp.zeros((ACCOUNTS, LANES), jnp.int16),) * parts
        )
        marks = []
        for part in range(parts):
            last = row_max(found[part])
            marks.append(jnp.where(last > 0, 1.0, 0.0))
            last_ref[part * LANES : (part + 1) * LANES, :] = short(column_of(last))

        def build(trip, count):
            for inner in range(step):
                at = lane_slice((trip * step + inner) * LANES)
                user, pos = stacked(user16_ref[:, at]), stacked(pos16_ref[:, at])
                grown = []
                for part in range(parts):
                    here = slice(part * LANES, (part + 1) * LANES)
                    weight = one_if((user == ids_of(part)) & (pos >= last_ref[here, :]))
                    mask_ref[here, at] = weight
                    grown.append(count[part] + weight)
                count = tuple(grown)
            return count

        count = lax.fori_loop(
            0, chunks // step, build, (jnp.zeros((ACCOUNTS, LANES), jnp.bfloat16),) * parts
        )
        total = jnp.dot(mask_ref[...], halves_ref[...], preferred_element_type=jnp.float32)
        total = total[:, 0:LANES] + total[:, LANES : 2 * LANES]
        for part in range(parts):
            owner = block * parts + part
            half, at = lax.rem(owner, 2), owner // 2
            state_ref[half, at, 0:8, :] = jnp.concatenate(
                [row_sum(count[part]), marks[part], jnp.zeros((6, LANES), jnp.float32)], axis=0
            )
            state_ref[half, at, 8:TILE, :] = total[part * ACCOUNTS : (part + 1) * ACCOUNTS]


def inside_sessions(
    first_block, end_block, halves_ref, user_ref, flagged16_ref, pos16_ref,
    sum_ref, count_ref, open_ref, key16_ref, mask_ref, keycol_ref, cnt_ref, acc_ref
):
    rows = acc_ref.shape[0]
    parts = rows // LANES
    diagonal = short(lax.broadcasted_iota(jnp.int32, (LANES, LANES), 1)) <= short(
        lax.broadcasted_iota(jnp.int32, (LANES, LANES), 0)
    )

    @pl.loop(first_block, end_block)
    def _(block):
        base = block * rows
        here = [slice(part * LANES, (part + 1) * LANES) for part in range(parts)]
        mine = [lane_slice(base + part * LANES) for part in range(parts)]
        for part in range(parts):
            keycol_ref[here[part], :] = short(column_of(user_ref[0:1, mine[part]]))

        def latest(trip, found):
            for inner in range(parts):
                at = lane_slice(trip * rows + inner * LANES)
                flagged, pos = stacked(flagged16_ref[:, at]), stacked(pos16_ref[:, at])
                found = tuple(
                    jnp.where(flagged == keycol_ref[here[part], :], pos, found[part])
                    for part in range(parts)
                )
            return found

        found = lax.fori_loop(
            0, block, latest, (jnp.zeros((LANES, LANES), jnp.int16),) * parts
        )
        keys = []
        for part in range(parts):
            seen = found[part]
            for inner in range(part + 1):
                same = stacked(flagged16_ref[:, mine[inner]]) == keycol_ref[here[part], :]
                if inner == part:
                    same = same & diagonal
                seen = jnp.where(same, stacked(pos16_ref[:, mine[inner]]), seen)
            start = row_max(seen)
            user = user_ref[0:1, mine[part]]
            key = jnp.where(start > 0, start, -1 - user)
            keys.append(key)
            open_ref[0:1, mine[part]] = jnp.where(start > 0, -1, user)
        for part in range(parts):
            keycol_ref[here[part], :] = short(column_of(keys[part]))
            key16_ref[:, mine[part]] = short(jnp.broadcast_to(keys[part], (16, LANES)))

        for part in range(parts):
            key = keycol_ref[here[part], :]
            count = jnp.zeros((LANES, LANES), jnp.bfloat16)
            for inner in range(parts):
                if inner > part:
                    mask_ref[here[part], here[inner]] = jnp.zeros((LANES, LANES), jnp.bfloat16)
                    continue
                same = stacked(key16_ref[:, mine[inner]]) == key
                if inner == part:
                    same = same & diagonal
                weight = one_if(same)
                mask_ref[here[part], here[inner]] = weight
                count = count + weight
            cnt_ref[here[part], :] = count
        acc_ref[...] = jnp.dot(
            mask_ref[0:rows, 0:rows],
            halves_ref[pl.ds(pl.multiple_of(base, rows), rows), :],
            preferred_element_type=jnp.float32,
        )

        @pl.loop(0, block)
        def _(trip):
            for part in range(parts):
                key = keycol_ref[here[part], :]
                count = cnt_ref[here[part], :]
                for inner in range(parts):
                    at = lane_slice(trip * rows + inner * LANES)
                    weight = one_if(stacked(key16_ref[:, at]) == key)
                    mask_ref[here[part], here[inner]] = weight
                    count = count + weight
                cnt_ref[here[part], :] = count
            acc_ref[...] += jnp.dot(
                mask_ref[0:rows, 0:rows],
                halves_ref[pl.ds(pl.multiple_of(trip * rows, rows), rows), :],
                preferred_element_type=jnp.float32,
            )

        sum_ref[pl.ds(pl.multiple_of(base, rows), rows), :] = (
            acc_ref[:, 0:LANES] + acc_ref[:, LANES : 2 * LANES]
        )
        for part in range(parts):
            count_ref[0:1, mine[part]] = row_sum(cnt_ref[here[part], :])


SPANS = ((0, 8 + ACCOUNTS // 2), (8 + ACCOUNTS // 2, TILE))


def follow(earlier, later, stats, part):
    mark = stats[1:2, :]
    carry_on = 1.0 - mark
    column = column_of(carry_on)
    if part:
        return later + column[ACCOUNTS // 2 :] * earlier
    sums = later[8:] + column[0 : ACCOUNTS // 2] * earlier[8:]
    count = later[0:1] + carry_on * earlier[0:1]
    seen = jnp.maximum(mark, earlier[1:2])
    return jnp.concatenate([count, seen, later[2:8], sums], axis=0)


def exchange(
    groups, owners, home_ref, account_ref, flag_ref, feature_ref,
    table_ref, count_ref, sum_ref, own_count_ref, open_ref,
    state_ref, halves, user_ref, user16, flagged16, pos16, key16, mask, last, keycol, cnt, acc,
    pair_in, chip, chip_in, time_out, time_in, back_out, back_in, pair_out, pair_back, sends, recvs,
):
    chips = owners // 2
    time, me = lax.axis_index("tm"), lax.axis_index("users")
    core, z = lax.rem(me, 2), me // 2
    sibling = me + 1 - 2 * core
    other = 1 - core

    def cut(ref, part, *at):
        return ref.at[(*at, pl.ds(SPANS[part][0], SPANS[part][1] - SPANS[part][0]))]

    def get(ref, part, *at):
        return ref[(*at, slice(*SPANS[part]), slice(None))]

    def put(ref, part, values, *at):
        ref[(*at, slice(*SPANS[part]), slice(None))] = values

    def stats(ref, *at):
        return ref[(*at, slice(0, 8), slice(None))]

    def empty(part):
        return jnp.zeros((SPANS[part][1] - SPANS[part][0], LANES), jnp.float32)

    def copy(source, target, stage, part, mine, theirs, device):
        return pltpu.make_async_remote_copy(
            src_ref=source,
            dst_ref=target,
            send_sem=sends.at[2 * stage + part, mine],
            recv_sem=recvs.at[2 * stage + part, theirs],
            device_id=device,
            device_id_type=pl.DeviceIdType.MESH,
        )

    def peer(shift):
        return lax.rem(z + shift, chips)

    def each(first, last, fn):
        if last - first <= 8:
            for index in range(first, last):
                fn(index)
        else:
            pl.loop(first, last)(fn)

    def device(group, user):
        return (group, user)

    barrier = pltpu.get_barrier_semaphore()
    pl.semaphore_signal(barrier, inc=1, device_id=device(time, sibling), device_id_type=pl.DeviceIdType.MESH)
    each(1, chips, lambda k: pl.semaphore_signal(
        barrier, inc=1, device_id=device(time, 2 * peer(k) + core), device_id_type=pl.DeviceIdType.MESH))
    each(1, groups, lambda k: pl.semaphore_signal(
        barrier, inc=1, device_id=device(lax.rem(time + k, groups), me), device_id_type=pl.DeviceIdType.MESH))

    prepare(home_ref, account_ref, flag_ref, feature_ref, halves, user_ref, user16, flagged16, pos16)
    closing_states(halves, user16, flagged16, pos16, state_ref, mask, last)
    blocks = sum_ref.shape[0] // acc.shape[0]

    def inside(first, end):
        inside_sessions(first, end, halves, user_ref, flagged16, pos16,
                        sum_ref, own_count_ref, open_ref, key16, mask, keycol, cnt, acc)

    pl.semaphore_wait(barrier, 1 + (chips - 1) + (groups - 1))

    first = core == 0
    shares = [blocks * n // 8 for n in (4, 5, 6)]

    def pair_copy(part, to):
        return copy(cut(state_ref, part, other, to), cut(pair_in, part, to), 0, part, to, to, device(time, sibling))

    for part in (0, 1):
        each(1, chips, lambda k: pair_copy(part, peer(k)).start())
        pair_copy(part, z).start()

    def to_owner(part, to):
        return copy(cut(chip, part, to), cut(chip_in, part, z), 1, part, to, z, device(time, 2 * to + core))

    def gather(part, to):
        pair_copy(part, to).wait_recv()
        mine, theirs = get(state_ref, part, core, to), get(pair_in, part, to)
        later = jnp.where(first, stats(pair_in, to), stats(state_ref, core, to))
        return follow(jnp.where(first, mine, theirs), jnp.where(first, theirs, mine), later, part)

    for part in (0, 1):
        def gather_send(k):
            to = peer(k)
            put(chip, part, gather(part, to), to)
            to_owner(part, to).start()

        each(1, chips, gather_send)
    for part in (0, 1):
        put(chip_in, part, gather(part, z), z)
    inside(0, shares[0])

    def to_time(part, k):
        to = lax.rem(time + k, groups)
        return copy(cut(time_out, part), cut(time_in, part, time), 2, part, to, time, device(to, me))

    for part in (0, 1):
        def from_owner(k):
            source = peer(k)
            copy(cut(chip, part, source), cut(chip_in, part, source), 1, part, source, source,
                 device(time, 2 * source + core)).wait_recv()

        each(1, chips, from_owner)
        put(time_out, part, lax.fori_loop(
            0, chips,
            lambda at, so_far: follow(so_far, get(chip_in, part, at), stats(chip_in, at), part),
            empty(part), unroll=chips <= 8))
        each(1, groups, lambda k: to_time(part, k).start())
        put(time_in, part, empty(part), time)
        inside(shares[part], shares[part + 1])

    def to_chip(part, to):
        return copy(cut(back_out, part, to), cut(back_in, part, z), 3, part, to, z, device(time, 2 * to + core))

    for part in (0, 1):
        def from_time(k):
            source = lax.rem(time + k, groups)
            copy(cut(time_out, part), cut(time_in, part, source), 2, part, source, source,
                 device(source, me)).wait_recv()

        each(1, groups, from_time)

        def advance(at, so_far):
            after = follow(so_far, get(time_in, part, at), stats(time_in, at), part)
            return jnp.where(at < time, after, so_far)

        def prefixes(at, so_far):
            put(back_out, part, so_far, at)
            return follow(so_far, get(chip_in, part, at), stats(chip_in, at), part)

        incoming = lax.fori_loop(0, groups, advance, empty(part), unroll=True)
        lax.fori_loop(0, chips, prefixes, incoming, unroll=chips <= 8)
        each(1, chips, lambda k: to_chip(part, peer(k)).start())
        put(back_in, part, get(back_out, part, z), z)
    inside(shares[2], blocks)

    def finish(half, part, at, tile):
        owner = 2 * at + half
        size = ACCOUNTS // 2
        start = pl.multiple_of(owner * ACCOUNTS + part * size, size)
        split_store(table_ref, pl.ds(start, size), tile if part else tile[8:])
        if part == 0:
            count_ref[0:1, lane_slice(owner * ACCOUNTS)] = tile[0:1]

    def to_sibling(part, at):
        return copy(cut(pair_out, part, at), cut(pair_back, part, at), 4, part, at, at, device(time, sibling))

    for part in (0, 1):
        def hand_over(k):
            at = peer(k)
            tile = get(back_in, part, at)
            before = jnp.where(first, get(state_ref, part, core, at), get(pair_in, part, at))
            marks = jnp.where(first, stats(state_ref, core, at), stats(pair_in, at))
            after = follow(tile, before, marks, part)
            put(pair_out, part, jnp.where(first, after, tile), at)
            to_sibling(part, at).start()
            finish(core, part, at, jnp.where(first, tile, after))

        def wait_hand_over(k):
            source = peer(k)
            copy(cut(back_out, part, source), cut(back_in, part, source), 3, part, source, source,
                 device(time, 2 * source + core)).wait_recv()
            hand_over(k)

        hand_over(0)
        each(1, chips, wait_hand_over)

    for part in (0, 1):
        def last_tile(k):
            at = peer(k)
            to_sibling(part, at).wait_recv()
            finish(other, part, at, get(pair_back, part, at))

        def drain(k):
            to_owner(part, peer(k)).wait_send()
            to_chip(part, peer(k)).wait_send()

        def drain_pair(k):
            pair_copy(part, peer(k)).wait_send()
            to_sibling(part, peer(k)).wait_send()

        each(0, chips, last_tile)
        each(1, chips, drain)
        each(0, chips, drain_pair)
        each(1, groups, lambda k: to_time(part, k).wait_send())


def means(open_ref, own_ref, sum_ref, table_ref, count_ref, out_ref, mask_ref):
    rows, users = mask_ref.shape
    high = (count_ref[...] * (1.0 / 32768.0)).astype(jnp.int32)
    low = count_ref[...].astype(jnp.int32) - high * 32768
    counts = []
    for part in range(rows // LANES):
        here = slice(part * LANES, (part + 1) * LANES)
        ids = short(column_of(open_ref[0:1, here]))

        def build(chunk, found, rows_of):
            at = lane_slice(chunk * LANES)
            same = short(jnp.broadcast_to(lane_ids(chunk * LANES), (LANES, LANES))) == ids
            mask_ref[here, at] = one_if(same)
            return tuple(
                jnp.where(same, short(jnp.broadcast_to(row, (LANES, LANES))), so_far)
                for row, so_far in zip(rows_of(chunk), found)
            )

        found = (jnp.zeros((LANES, LANES), jnp.int16),) * 2
        if users <= 1024:
            for chunk in range(users // LANES):
                at = slice(chunk * LANES, (chunk + 1) * LANES)
                found = build(chunk, found, lambda chunk: (high[:, at], low[:, at]))
        else:
            def pieces(chunk):
                count = count_ref[0:1, lane_slice(chunk * LANES)]
                upper = (count * (1.0 / 32768.0)).astype(jnp.int32)
                return upper, count.astype(jnp.int32) - upper * 32768

            found = lax.fori_loop(
                0, users // LANES, lambda chunk, found: build(chunk, found, pieces), found
            )
        count = found[0].astype(jnp.int32) * 32768 + found[1].astype(jnp.int32)
        counts.append(row_sum(count) + own_ref[0:1, here])
    before = jnp.dot(mask_ref[...], table_ref[...], preferred_element_type=jnp.float32)
    before = before[:, 0:LANES] + before[:, LANES : 2 * LANES]
    for part in range(rows // LANES):
        here = slice(part * LANES, (part + 1) * LANES)
        out_ref[here, :] = (sum_ref[here, :] + before[here]) / column_of(counts[part])


def body(groups, owners, features, home, account, flags):
    events = features.shape[0]
    users = owners * ACCOUNTS
    chips = owners // 2
    rows = math.gcd(events, 512)
    tall = math.gcd(events, 1024)
    group = math.gcd(users, 512)
    whole = pl.BlockSpec(memory_space=pltpu.VMEM)
    tiles = lambda *count: pltpu.VMEM((*count, TILE, LANES), jnp.float32)
    lots = max(chips, groups)
    table, prefix_count, own_sum, own_count, open_user = pl.pallas_call(
        functools.partial(exchange, groups, owners),
        out_shape=(
            jax.ShapeDtypeStruct((users, 2 * LANES), jnp.bfloat16),
            jax.ShapeDtypeStruct((1, users), jnp.float32),
            jax.ShapeDtypeStruct((events, LANES), jnp.float32),
            jax.ShapeDtypeStruct((1, events), jnp.float32),
            jax.ShapeDtypeStruct((1, events), jnp.int32),
        ),
        in_specs=[whole] * 4,
        out_specs=(whole,) * 5,
        scratch_shapes=[
            tiles(2, chips),
            pltpu.VMEM((events, 2 * LANES), jnp.bfloat16),
            pltpu.VMEM((1, events), jnp.int32),
            pltpu.VMEM((16, events), jnp.int16),
            pltpu.VMEM((16, events), jnp.int16),
            pltpu.VMEM((16, events), jnp.int16),
            pltpu.VMEM((16, events), jnp.int16),
            pltpu.VMEM((group, events), jnp.bfloat16),
            pltpu.VMEM((group, LANES), jnp.int16),
            pltpu.VMEM((rows, LANES), jnp.int16),
            pltpu.VMEM((rows, LANES), jnp.bfloat16),
            pltpu.VMEM((rows, 2 * LANES), jnp.float32),
            tiles(chips), tiles(chips), tiles(chips),
            tiles(), tiles(groups),
            tiles(chips), tiles(chips), tiles(chips), tiles(chips),
            pltpu.SemaphoreType.DMA((10, lots)),
            pltpu.SemaphoreType.DMA((10, lots)),
        ],
        compiler_params=pltpu.CompilerParams(
            collective_id=0, has_side_effects=True, vmem_limit_bytes=VMEM_LIMIT
        ),
        name="exchange",
    )(home.reshape(1, events), account.reshape(1, events), flags.reshape(1, events), features)

    return pl.pallas_call(
        means,
        grid=(events // tall,),
        out_shape=jax.ShapeDtypeStruct((events, LANES), jnp.float32),
        in_specs=[
            pl.BlockSpec((1, tall), lambda i: (0, i)),
            pl.BlockSpec((1, tall), lambda i: (0, i)),
            pl.BlockSpec((tall, LANES), lambda i: (i, 0)),
            pl.BlockSpec((users, 2 * LANES), lambda i: (0, 0)),
            pl.BlockSpec((1, users), lambda i: (0, 0)),
        ],
        out_specs=pl.BlockSpec((tall, LANES), lambda i: (i, 0)),
        scratch_shapes=[pltpu.VMEM((tall, users), jnp.bfloat16)],
        compiler_params=pltpu.CompilerParams(vmem_limit_bytes=VMEM_LIMIT),
        name="means",
    )(open_user, own_count, own_sum, table, prefix_count)


def solution(mesh):
    return jax.shard_map(
        functools.partial(body, mesh.shape["tm"], mesh.shape["users"]),
        mesh=mesh,
        in_specs=(
            P(("tm", "users"), None),
            P(("tm", "users"), None),
            P(("tm", "users")),
            P(("tm", "users")),
        ),
        out_specs=P(("tm", "users"), None),
        check_vma=False,
    )
```
